32 devices in a mesh: replica: 4 (over y, x), fsdp: 8 (over z, core).
Axes of the slice: x: 2, y: 2, z: 4, core: 2. Of those that a mesh axis runs over, the one named last changes fastest.
Arguments:
- codes: int32 [4, 8192, 4096], P('replica', None, 'fsdp'), may hold values from -127 to 127
- scales: float32 [4, 32, 8192], P('replica', 'fsdp'), may hold values from 0.002 to 0.03
- master: float32 [8192, 4096], P(('replica', 'fsdp')), may hold values from -6 to 6
- momentum: float32 [8192, 4096], P(('replica', 'fsdp')), may hold values from -6 to 6
Outputs:
- new_master: float32 [8192, 4096], P(('replica', 'fsdp'))
- new_momentum: float32 [8192, 4096], P(('replica', 'fsdp'))
- weights: bfloat16 [8192, 4096], P(None, 'fsdp')
The draws below stay inside these ranges and needn't reach their ends.
All inputs are finite; a program needn't handle non-finite values.
Results may differ from the reference program's by a relative error of at most 0.0075.
Values may be sent and summed in bfloat16 or wider, within the bound.
A program may use at most 128 MiB of HBM per device.

```python
import math
import jax
import jax.numpy as jnp
from jax import lax

D = 4096
FF = 8192
BLOCK = 128
REPLICAS = 4
N_REPLICA = 4


def place_ends(entries, key, least, high):
    shape = entries.shape
    spot = [jax.random.randint(jax.random.fold_in(key, axis), (), 0, shape[axis]) for axis in range(len(shape))]
    entries = entries.at[tuple(spot)].set(least)
    longest = shape.index(max(shape))
    spot[longest] = (spot[longest] + 1) % shape[longest]
    return entries.at[tuple(spot)].set(high)


def block_scale(stream_key, extent, cuts, low, top_value):
    def one(dim, blocks):
        steps = jax.random.uniform(jax.random.fold_in(jax.random.fold_in(stream_key, 6), dim), (blocks,), jnp.float32, low / len(cuts), top_value / len(cuts))
        return jnp.repeat(jnp.exp(steps), extent[dim] // blocks).reshape((-1,) + (1,) * (len(extent) - dim - 1))

    loudness = one(*cuts[0])
    for cut in cuts[1:]:
        loudness = loudness * one(*cut)
    return loudness


def noise(stream_key, extent, width, limit, split=(), held_as=jnp.bfloat16):
    entries = width * jax.random.normal(stream_key, extent, jnp.float32)
    if split:
        entries = entries * block_scale(stream_key, extent, split, -0.22, 0.18)
    return jnp.clip(entries, -limit, limit).astype(held_as)


def setup_inputs(seed: int = 0) -> dict:
    seeds = jax.random.split(jax.random.key(seed), 5)
    codes = place_ends(jax.random.randint(seeds[0], (REPLICAS, FF, D), -127, 128), jax.random.fold_in(seeds[0], 1), -127, 127).astype(jnp.int32)
    scales = jnp.clip(jnp.exp(math.log(0.03) - 2.70805 * jax.random.uniform(seeds[1], (REPLICAS, D // BLOCK, FF), jnp.float32) ** block_scale(seeds[1], (REPLICAS, D // BLOCK, FF), ((0, 4), (1, 8)), -0.2, 0.2)), 0.002, 0.03)
    master = noise(seeds[2], (FF, D), 1.0, 6.0, ((0, 32),), jnp.float32)
    momentum = noise(seeds[3], (FF, D), 0.5, 6.0, ((0, 32),), jnp.float32)
    return {"codes": codes, "scales": scales, "master": master, "momentum": momentum}


outer_rate = 0.7
momentum_factor = 0.9


def reference(codes, scales, master, momentum):
    def add_worker(replica_index, running):
        quantized = lax.dynamic_index_in_dim(codes, replica_index, 0, keepdims=False).astype(jnp.float32)
        scale_rows = lax.dynamic_index_in_dim(scales, replica_index, 0, keepdims=False)
        block_count = scale_rows.shape[0]
        dequantized = quantized.reshape(FF, block_count, BLOCK) * jnp.transpose(scale_rows)[:, :, None]
        return running + dequantized.reshape(FF, D)

    summed = lax.fori_loop(0, N_REPLICA, add_worker, jnp.zeros((FF, D), jnp.float32))
    mean_delta = summed / N_REPLICA
    new_momentum = momentum_factor * momentum + mean_delta
    new_master = master - outer_rate * (mean_delta + momentum_factor * new_momentum)
    weights = new_master.astype(jnp.bfloat16)
    return (new_master, new_momentum, weights)
```

```python
import functools

import jax
import jax.numpy as jnp
from jax import lax
from jax.experimental import pallas as pl
from jax.experimental.pallas import tpu as pltpu
from jax.sharding import PartitionSpec as P

MESH = pl.DeviceIdType.MESH

outer_rate = 0.7
momentum_factor = 0.9

LAGS = (0, 2, 3, 4, 5, 6, 7)
RS1, RS2, X1, X2, AG1, AG2 = range(6)


def kernel(cfg, codes, scales, master, momentum, new_master, new_momentum, weights,
           delta, rs1e, rs1o, rs2e, rs2o, part, got, wsend, wbuf, mast, mom, cbuf, sbuf,
           send_sem, recv_sem, in_sem, state_sem, out_sem):
    A, B, F, K, sub, width, blocks = cfg
    R, FS, block = A * B, F * sub, width // blocks
    r, f = lax.axis_index("replica"), lax.axis_index("fsdp")
    a, b = r // B, lax.rem(r, B)

    def a_peer(i):
        return lax.rem(a + 1 + i, A)

    def b_peer(i):
        return lax.rem(b + 1 + i, B)

    def f_peer(i):
        return lax.rem(f + 1 + i, F)

    def load(k):
        slot = lax.rem(k, 2)
        return (
            pltpu.make_async_copy(codes.at[:, k], cbuf.at[slot], in_sem.at[0, slot]),
            pltpu.make_async_copy(scales.at[:, k], sbuf.at[slot], in_sem.at[1, slot]),
        )

    for k in range(min(2, K)):
        for copy in load(k):
            copy.start()
    state_in = (
        pltpu.make_async_copy(master, mast, state_sem.at[0]),
        pltpu.make_async_copy(momentum, mom, state_sem.at[1]),
    )
    for copy in state_in:
        copy.start()

    barrier = pltpu.get_barrier_semaphore()
    for i in range(A - 1):
        pl.semaphore_signal(barrier, inc=1, device_id=(a_peer(i) * B + b, f), device_id_type=MESH)
    for i in range(B - 1):
        pl.semaphore_signal(barrier, inc=1, device_id=(a * B + b_peer(i), f), device_id_type=MESH)
    for i in range(F - 1):
        pl.semaphore_signal(barrier, inc=1, device_id=(r, f_peer(i)), device_id_type=MESH)
    pl.semaphore_wait(barrier, A + B + F - 3)

    def send(stage, k, src, dst, device):
        pltpu.make_async_remote_copy(
            src_ref=src, dst_ref=dst, send_sem=send_sem.at[stage, k], recv_sem=recv_sem.at[stage, k],
            device_id=device, device_id_type=MESH,
        ).start()

    def wait_bytes(sem, stage, k, ref):
        pltpu.make_async_copy(ref, ref, sem.at[stage, k]).wait()

    def rows(j):
        return pl.ds(pl.multiple_of(j * sub, sub), sub)

    def f32(x):
        return x.astype(jnp.float32)

    def amount(stage, k, even):
        if stage == RS1:
            return rs1e.at[k // 2] if even else rs1o.at[k // 2]
        if stage == RS2:
            return rs2e.at[k // 2] if even else rs2o.at[k // 2]
        if stage in (X1, X2):
            return part.at[k, pl.ds(0, (F - 1) * sub)]
        first, second = (B - 1, B * (A - 1)) if even else (A - 1, A * (B - 1))
        count = first if stage == AG1 else second
        return delta.at[k, pl.ds(0, count)]

    def by_parity(k, fn):
        @pl.when(lax.rem(k, 2) == 0)
        def _():
            fn(True)

        if K > 1:
            @pl.when(lax.rem(k, 2) == 1)
            def _():
                fn(False)

    def stage0(k):
        slot = lax.rem(k, 2)
        for copy in load(k):
            copy.wait()

        def one(g, carry):
            q, j = g // F, lax.rem(g, F)
            for n in range(blocks):
                cols = pl.ds(n * block, block)
                value = f32(cbuf[slot, g, :, cols]) * sbuf[slot, g, :, pl.ds(n, 1)]
                delta[k, q, rows(j), cols] = value.astype(jnp.bfloat16)
            return carry

        lax.fori_loop(0, R * F, one, 0)

        @pl.when(k + 2 < K)
        def _():
            for copy in load(k + 2):
                copy.start()

        def go(even):
            if even:
                for i in range(B - 1):
                    bb = b_peer(i)
                    for aa in range(A):
                        send(RS1, k, delta.at[k, aa * B + bb], rs1e.at[k // 2, B - 2 - i, aa], (a * B + bb, f))
            else:
                for i in range(A - 1):
                    aa = a_peer(i)
                    send(RS1, k, delta.at[k, pl.ds(aa * B, B)], rs1o.at[k // 2, A - 2 - i], (aa * B + b, f))

        by_parity(k, go)

    def stage1(k):
        def go(even):
            wait_bytes(recv_sem, RS1, k, amount(RS1, k, even))
            buf, count, peers = (rs1e, B - 1, A - 1) if even else (rs1o, A - 1, B - 1)
            for i in range(peers):
                q = a_peer(i) if even else b_peer(i)
                target = q * B + b if even else a * B + q

                def add(j, carry):
                    total = f32(delta[k, target, rows(j), :])
                    for s in range(count):
                        total = total + f32(buf[k // 2, s, q, rows(j), :])
                    buf[k // 2, 0, q, rows(j), :] = total.astype(jnp.bfloat16)
                    return carry

                lax.fori_loop(0, F, add, 0)
                dst = rs2e if even else rs2o
                send(RS2, k, buf.at[k // 2, 0, q], dst.at[k // 2, peers - 1 - i], (target, f))

        by_parity(k, go)

    def stage2(k):
        def go(even):
            wait_bytes(recv_sem, RS2, k, amount(RS2, k, even))
            one, two = (rs1e, rs2e) if even else (rs1o, rs2o)
            ones, twos = (B - 1, A - 1) if even else (A - 1, B - 1)
            q = a if even else b

            def add(j, carry):
                total = f32(delta[k, r, rows(j), :])
                for s in range(ones):
                    total = total + f32(one[k // 2, s, q, rows(j), :])
                for s in range(twos):
                    total = total + f32(two[k // 2, s, rows(j), :])
                part[k, rows(j), :] = total.astype(jnp.bfloat16)
                return carry

            lax.fori_loop(0, F, add, 0)

        by_parity(k, go)

        def out(i, carry):
            j = f_peer(i)
            send(X1, k, part.at[k, rows(j)], got.at[k, rows(f)], (r, j))
            return carry

        lax.fori_loop(0, F - 1, out, 0)
        got[k, rows(f), :] = part[k, rows(f), :]

    def results(k):
        span = pl.ds(pl.multiple_of(k * sub, sub), sub)
        return (
            pltpu.make_async_copy(mast.at[span], new_master.at[span], out_sem.at[0, k]),
            pltpu.make_async_copy(mom.at[span], new_momentum.at[span], out_sem.at[1, k]),
        )

    def stage3(k):
        @pl.when(k == 0)
        def _():
            for copy in state_in:
                copy.wait()

        wait_bytes(recv_sem, X1, k, amount(X1, k, True))
        span = pl.ds(pl.multiple_of(k * sub, sub), sub)

        def update(j, carry):
            cols = pl.ds(pl.multiple_of(j * width, width), width)
            mean = f32(got[k, rows(j), :]) * (1.0 / R)
            m = momentum_factor * mom[span, cols] + mean
            p = mast[span, cols] - outer_rate * (mean + momentum_factor * m)
            mom[span, cols] = m
            mast[span, cols] = p
            wsend[k, rows(j), :] = p.astype(jnp.bfloat16)
            return carry

        lax.fori_loop(0, F, update, 0)

        def out(i, carry):
            j = f_peer(i)
            send(X2, k, wsend.at[k, rows(j)], wbuf.at[k, r, rows(f)], (r, j))
            return carry

        lax.fori_loop(0, F - 1, out, 0)
        wbuf[k, r, rows(f), :] = wsend[k, rows(f), :]
        for copy in results(k):
            copy.start()

    def stage4(k):
        wait_bytes(recv_sem, X2, k, amount(X2, k, True))

        def go(even):
            here = wbuf.at[k, r]
            for i in range(B - 1 if even else A - 1):
                target = a * B + b_peer(i) if even else a_peer(i) * B + b
                send(AG1, k, here, here, (target, f))

        by_parity(k, go)

    def stage5(k):
        def go(even):
            wait_bytes(recv_sem, AG1, k, amount(AG1, k, even))
            if even:
                here = wbuf.at[k, pl.ds(a * B, B)]
                for i in range(A - 1):
                    send(AG2, k, here, here, (a_peer(i) * B + b, f))
            else:
                for i in range(B - 1):
                    for aa in range(A):
                        here = wbuf.at[k, aa * B + b]
                        send(AG2, k, here, here, (a * B + b_peer(i), f))

        by_parity(k, go)

    def columns(k, q):
        return pltpu.make_async_copy(
            wbuf.at[k, q].reshape(F, sub, width), weights.at[pl.ds(q * F, F), k], out_sem.at[2 + q, k]
        )

    def stage6(k):
        by_parity(k, lambda even: wait_bytes(recv_sem, AG2, k, amount(AG2, k, even)))
        for q in range(R):
            columns(k, q).start()

    stages = (stage0, stage1, stage2, stage3, stage4, stage5, stage6)

    def step(t, carry):
        for lag, stage in zip(LAGS, stages):
            k = t - lag

            @pl.when((k >= 0) & (k < K))
            def _():
                stage(k)

        return carry

    lax.fori_loop(0, K + LAGS[-1], step, 0)

    def finish(k, carry):
        for copy in results(k):
            copy.wait()
        for q in range(R):
            columns(k, q).wait()

        def go(even):
            for stage in range(6):
                wait_bytes(send_sem, stage, k, amount(stage, k, even))

        by_parity(k, go)
        return carry

    lax.fori_loop(0, K, finish, 0)


def solution(mesh):
    R, F = mesh.shape["replica"], mesh.shape["fsdp"]
    B = 2
    A = R // B

    def local(codes, scales, master, momentum):
        total_rows, width = codes.shape[1:]
        blocks = scales.shape[1]
        own = total_rows // (R * F)
        sub = 32 if own % 32 == 0 else own
        K = own // sub
        FS = F * sub
        even, odd = (K + 1) // 2, max(1, K // 2)
        codes = codes.reshape(R * F, K, sub, width)
        scales = jnp.transpose(scales[0]).reshape(R * F, K, sub, blocks)
        any_spec = pl.BlockSpec(memory_space=pl.ANY)
        bf16 = jnp.bfloat16
        new_master, new_momentum, weights = pl.pallas_call(
            functools.partial(kernel, (A, B, F, K, sub, width, blocks)),
            out_shape=(
                jax.ShapeDtypeStruct(master.shape, jnp.float32),
                jax.ShapeDtypeStruct(momentum.shape, jnp.float32),
                jax.ShapeDtypeStruct((R * F, K, sub, width), bf16),
            ),
            in_specs=[any_spec] * 4,
            out_specs=(any_spec,) * 3,
            scratch_shapes=[
                pltpu.VMEM((K, R, FS, width), bf16),
                pltpu.VMEM((even, B - 1, A, FS, width), bf16),
                pltpu.VMEM((odd, A - 1, B, FS, width), bf16),
                pltpu.VMEM((even, A - 1, FS, width), bf16),
                pltpu.VMEM((odd, B - 1, FS, width), bf16),
                pltpu.VMEM((K, FS, width), bf16),
                pltpu.VMEM((K, FS, width), bf16),
                pltpu.VMEM((K, FS, width), bf16),
                pltpu.VMEM((K, R, FS, width), bf16),
                pltpu.VMEM(master.shape, jnp.float32),
                pltpu.VMEM(momentum.shape, jnp.float32),
                pltpu.VMEM((2, R * F, sub, width), jnp.int32),
                pltpu.VMEM((2, R * F, sub, blocks), jnp.float32),
                pltpu.SemaphoreType.DMA((6, K)),
                pltpu.SemaphoreType.DMA((6, K)),
                pltpu.SemaphoreType.DMA((2, 2)),
                pltpu.SemaphoreType.DMA((2,)),
                pltpu.SemaphoreType.DMA((2 + R, K)),
            ],
            compiler_params=pltpu.CompilerParams(
                collective_id=0, has_side_effects=True, vmem_limit_bytes=60 * 1024 * 1024
            ),
        )(codes, scales, master, momentum)
        return (new_master, new_momentum, weights.reshape(total_rows, width))

    return jax.shard_map(
        local,
        mesh=mesh,
        in_specs=(
            P("replica", None, "fsdp"),
            P("replica", "fsdp", None),
            P(("replica", "fsdp"), None),
            P(("replica", "fsdp"), None),
        ),
        out_specs=(P(("replica", "fsdp"), None), P(("replica", "fsdp"), None), P(None, "fsdp")),
        check_vma=False,
    )
```

```python
import functools

import jax
import jax.numpy as jnp
from jax import lax
from jax.experimental import pallas as pl
from jax.experimental.pallas import tpu as pltpu
from jax.sharding import PartitionSpec as P

MESH = pl.DeviceIdType.MESH

outer_rate = 0.7
momentum_factor = 0.9

LAGS = (0, 2, 4, 6, 8, 10, 12)
RS1, RS2, X1, X2, AG1, AG2 = range(6)


def kernel(cfg, codes, scales, master, momentum, new_master, new_momentum, weights,
           delta, rs1e, rs1o, rs2e, rs2o, part, got, wsend, mast, mom, cbuf, flat, sbuf,
           send_sem, recv_sem, in_sem, state_sem, out_sem, own_sem):
    A, B, F, K, sub, width, blocks = cfg
    R, FS, block = A * B, F * sub, width // blocks
    r, f = lax.axis_index("replica"), lax.axis_index("fsdp")
    a, b = r // B, lax.rem(r, B)

    def a_peer(i):
        return lax.rem(a + 1 + i, A)

    def b_peer(i):
        return lax.rem(b + 1 + i, B)

    def f_peer(i):
        return lax.rem(f + 1 + i, F)

    def load(k):
        slot = lax.rem(k, 2)
        return (pltpu.make_async_copy(codes.at[:, k], cbuf.at[slot], in_sem.at[slot]),)

    scales_in = pltpu.make_async_copy(scales.at[0], flat.at[pl.ds(0, blocks)], state_sem.at[2])
    scales_in.start()
    for k in range(min(2, K)):
        for copy in load(k):
            copy.start()
    state_in = (
        pltpu.make_async_copy(master, mast, state_sem.at[0]),
        pltpu.make_async_copy(momentum, mom, state_sem.at[1]),
    )
    for copy in state_in:
        copy.start()

    barrier = pltpu.get_barrier_semaphore()
    for i in range(A - 1):
        pl.semaphore_signal(barrier, inc=1, device_id=(a_peer(i) * B + b, f), device_id_type=MESH)
    for i in range(B - 1):
        pl.semaphore_signal(barrier, inc=1, device_id=(a * B + b_peer(i), f), device_id_type=MESH)
    for i in range(F - 1):
        pl.semaphore_signal(barrier, inc=1, device_id=(r, f_peer(i)), device_id_type=MESH)
    scales_in.wait()

    def turn(i, carry):
        tile = flat[:, pl.ds(pl.multiple_of(i * 128, 128), 128)]
        sbuf[pl.ds(pl.multiple_of(i * 128, 128), 128), :] = jnp.transpose(tile)
        return carry

    lax.fori_loop(0, flat.shape[1] // 128, turn, 0, unroll=8)
    pl.semaphore_wait(barrier, A + B + F - 3)

    def send(stage, k, src, dst, device):
        pltpu.make_async_remote_copy(
            src_ref=src, dst_ref=dst, send_sem=send_sem.at[stage, k], recv_sem=recv_sem.at[stage, k],
            device_id=device, device_id_type=MESH,
        ).start()

    def wait_bytes(sem, stage, k, ref):
        pltpu.make_async_copy(ref, ref, sem.at[stage, k]).wait()

    def rows(j):
        return pl.ds(pl.multiple_of(j * sub, sub), sub)

    def f32(x):
        return x.astype(jnp.float32)

    def amount(stage, k, even):
        if stage == RS1:
            return rs1e.at[k // 2] if even else rs1o.at[k // 2]
        if stage == RS2:
            return rs2e.at[k // 2] if even else rs2o.at[k // 2]
        if stage in (X1, X2):
            return part.at[k, pl.ds(0, (F - 1) * sub)]
        first, second = (B - 1, B * (A - 1)) if even else (A - 1, A * (B - 1))
        count = first if stage == AG1 else second
        return delta.at[k, pl.ds(0, count)]

    def by_parity(k, fn):
        @pl.when(lax.rem(k, 2) == 0)
        def _():
            fn(True)

        if K > 1:
            @pl.when(lax.rem(k, 2) == 1)
            def _():
                fn(False)

    def stage0(k):
        slot = lax.rem(k, 2)
        for copy in load(k):
            copy.wait()

        def one(g, carry):
            q, j = g // F, lax.rem(g, F)
            for n in range(blocks):
                cols = pl.ds(n * block, block)
                value = f32(cbuf[slot, g, :, cols]) * sbuf[pl.ds(pl.multiple_of((g * K + k) * sub, sub), sub), pl.ds(n, 1)]
                delta[k, q, rows(j), cols] = value.astype(jnp.bfloat16)
            return carry

        lax.fori_loop(0, R * F, one, 0, unroll=4)

        @pl.when(k + 2 < K)
        def _():
            for copy in load(k + 2):
                copy.start()

        def go(even):
            if even:
                for i in range(B - 1):
                    bb = b_peer(i)
                    for aa in range(A):
                        send(RS1, k, delta.at[k, aa * B + bb], rs1e.at[k // 2, B - 2 - i, aa], (a * B + bb, f))
            else:
                for i in range(A - 1):
                    aa = a_peer(i)
                    send(RS1, k, delta.at[k, pl.ds(aa * B, B)], rs1o.at[k // 2, A - 2 - i], (aa * B + b, f))

        by_parity(k, go)

    def stage1(k):
        def go(even):
            wait_bytes(recv_sem, RS1, k, amount(RS1, k, even))
            buf, count, peers = (rs1e, B - 1, A - 1) if even else (rs1o, A - 1, B - 1)
            for i in range(peers):
                q = a_peer(i) if even else b_peer(i)
                target = q * B + b if even else a * B + q

                def add(j, carry):
                    total = f32(delta[k, target, rows(j), :])
                    for s in range(count):
                        total = total + f32(buf[k // 2, s, q, rows(j), :])
                    buf[k // 2, 0, q, rows(j), :] = total.astype(jnp.bfloat16)
                    return carry

                lax.fori_loop(0, F, add, 0, unroll=4)
                dst = rs2e if even else rs2o
                send(RS2, k, buf.at[k // 2, 0, q], dst.at[k // 2, peers - 1 - i], (target, f))

        by_parity(k, go)

    def stage2(k):
        def go(even):
            wait_bytes(recv_sem, RS2, k, amount(RS2, k, even))
            one, two = (rs1e, rs2e) if even else (rs1o, rs2o)
            ones, twos = (B - 1, A - 1) if even else (A - 1, B - 1)
            q = a if even else b

            def add(j, carry):
                total = f32(delta[k, r, rows(j), :])
                for s in range(ones):
                    total = total + f32(one[k // 2, s, q, rows(j), :])
                for s in range(twos):
                    total = total + f32(two[k // 2, s, rows(j), :])
                part[k, rows(j), :] = total.astype(jnp.bfloat16)
                return carry

            lax.fori_loop(0, F, add, 0, unroll=4)

        by_parity(k, go)

        def out(i, carry):
            j = f_peer(i)
            send(X1, k, part.at[k, rows(j)], got.at[k, rows(f)], (r, j))
            return carry

        lax.fori_loop(0, F - 1, out, 0)
        got[k, rows(f), :] = part[k, rows(f), :]

    def results(k):
        span = pl.ds(pl.multiple_of(k * sub, sub), sub)
        return (
            pltpu.make_async_copy(mast.at[span], new_master.at[span], out_sem.at[0, k]),
            pltpu.make_async_copy(mom.at[span], new_momentum.at[span], out_sem.at[1, k]),
        )

    def own(k):
        return pltpu.make_async_copy(wsend.at[k, rows(f)], weights.at[r * F + f, k], own_sem.at[k])

    def stage3(k):
        @pl.when(k == 0)
        def _():
            for copy in state_in:
                copy.wait()

        wait_bytes(recv_sem, X1, k, amount(X1, k, True))
        span = pl.ds(pl.multiple_of(k * sub, sub), sub)

        def update(j, carry):
            cols = pl.ds(pl.multiple_of(j * width, width), width)
            mean = f32(got[k, rows(j), :]) * (1.0 / R)
            m = momentum_factor * mom[span, cols] + mean
            p = mast[span, cols] - outer_rate * (mean + momentum_factor * m)
            mom[span, cols] = m
            mast[span, cols] = p
            wsend[k, rows(j), :] = p.astype(jnp.bfloat16)
            return carry

        lax.fori_loop(0, F, update, 0, unroll=4)

        def out(i, carry):
            j = f_peer(i)
            send(X2, k, wsend.at[k, rows(j)], weights.at[r * F + f, k], (r, j))
            return carry

        lax.fori_loop(0, F - 1, out, 0)
        own(k).start()
        for copy in results(k):
            copy.start()

    def stage4(k):
        wait_bytes(recv_sem, X2, k, amount(X2, k, True))
        own(k).wait()

        def go(even):
            here = weights.at[pl.ds(r * F, F), k]
            for i in range(B - 1 if even else A - 1):
                target = a * B + b_peer(i) if even else a_peer(i) * B + b
                send(AG1, k, here, here, (target, f))

        by_parity(k, go)

    def stage5(k):
        def go(even):
            wait_bytes(recv_sem, AG1, k, amount(AG1, k, even))
            if even:
                here = weights.at[pl.ds(a * B * F, B * F), k]
                for i in range(A - 1):
                    send(AG2, k, here, here, (a_peer(i) * B + b, f))
            else:
                for i in range(B - 1):
                    for aa in range(A):
                        here = weights.at[pl.ds((aa * B + b) * F, F), k]
                        send(AG2, k, here, here, (a * B + b_peer(i), f))

        by_parity(k, go)

    def stage6(k):
        by_parity(k, lambda even: wait_bytes(recv_sem, AG2, k, amount(AG2, k, even)))

    stages = (stage0, stage1, stage2, stage3, stage4, stage5, stage6)

    def step(t, carry):
        for lag, stage in zip(LAGS, stages):
            k = t - lag

            @pl.when((k >= 0) & (k < K))
            def _():
                stage(k)

        return carry

    lax.fori_loop(0, K + LAGS[-1], step, 0)

    def finish(k, carry):
        for copy in results(k):
            copy.wait()

        def go(even):
            for stage in range(6):
                wait_bytes(send_sem, stage, k, amount(stage, k, even))

        by_parity(k, go)
        return carry

    lax.fori_loop(0, K, finish, 0)


def solution(mesh):
    R, F = mesh.shape["replica"], mesh.shape["fsdp"]
    B = 2
    A = R // B

    def local(codes, scales, master, momentum):
        total_rows, width = codes.shape[1:]
        blocks = scales.shape[1]
        own = total_rows // (R * F)
        sub = 16 if own % 16 == 0 else own
        K = own // sub
        FS = F * sub
        even, odd = (K + 1) // 2, max(1, K // 2)
        codes = codes.reshape(R * F, K, sub, width)
        lines = max(8, blocks)
        any_spec = pl.BlockSpec(memory_space=pl.ANY)
        bf16 = jnp.bfloat16
        new_master, new_momentum, weights = pl.pallas_call(
            functools.partial(kernel, (A, B, F, K, sub, width, blocks)),
            out_shape=(
                pltpu.VMEM(master.shape, jnp.float32),
                pltpu.VMEM(momentum.shape, jnp.float32),
                pltpu.VMEM((R * F, K, sub, width), bf16),
            ),
            in_specs=[any_spec] * 4,
            out_specs=(any_spec,) * 3,
            scratch_shapes=[
                pltpu.VMEM((K, R, FS, width), bf16),
                pltpu.VMEM((even, B - 1, A, FS, width), bf16),
                pltpu.VMEM((odd, A - 1, B, FS, width), bf16),
                pltpu.VMEM((even, A - 1, FS, width), bf16),
                pltpu.VMEM((odd, B - 1, FS, width), bf16),
                pltpu.VMEM((K, FS, width), bf16),
                pltpu.VMEM((K, FS, width), bf16),
                pltpu.VMEM((K, FS, width), bf16),
                pltpu.VMEM(master.shape, jnp.float32),
                pltpu.VMEM(momentum.shape, jnp.float32),
                pltpu.VMEM((2, R * F, sub, width), jnp.int32),
                pltpu.VMEM((lines, total_rows), jnp.float32),
                pltpu.VMEM((total_rows, lines), jnp.float32),
                pltpu.SemaphoreType.DMA((6, K)),
                pltpu.SemaphoreType.DMA((6, K)),
                pltpu.SemaphoreType.DMA((2,)),
                pltpu.SemaphoreType.DMA((3,)),
                pltpu.SemaphoreType.DMA((2, K)),
                pltpu.SemaphoreType.DMA((K,)),
            ],
            compiler_params=pltpu.CompilerParams(
                collective_id=0, has_side_effects=True, vmem_limit_bytes=40 * 1024 * 1024
            ),
        )(codes, scales, master, momentum)
        return (new_master, new_momentum, weights.reshape(total_rows, width))

    return jax.shard_map(
        local,
        mesh=mesh,
        in_specs=(
            P("replica", None, "fsdp"),
            P("replica", "fsdp", None),
            P(("replica", "fsdp"), None),
            P(("replica", "fsdp"), None),
        ),
        out_specs=(P(("replica", "fsdp"), None), P(("replica", "fsdp"), None), P(None, "fsdp")),
        check_vma=False,
    )
```
